32 devices in a mesh: groups: 2 (over y), expert: 4 (over z), tensor: 4 (over x, core).
Axes of the slice: x: 2, y: 2, z: 4, core: 2. Of those that a mesh axis runs over, the one named last changes fastest.
Arguments:
- tokens: bfloat16 [256, 4096], P(('groups', 'expert'), 'tensor'), parts along dimension 0, may hold values from -6 to 6
- expert_ids: int32 [256, 8], P(('groups', 'expert')), parts along dimension 0, may hold values from 0 to 63, all different within a row; in each aligned block of 32 rows (0 to 31, 32 to 63, ...) at most 8 rows name the same one
- gate_fixed: int32 [256, 8], P(('groups', 'expert')), parts along dimension 0, may hold values from 1 to 65535
- w_gate: bfloat16 [64, 4096, 768], P('expert', None, 'tensor'), may hold values from -0.09375 to 0.09375
- w_up: bfloat16 [64, 4096, 768], P('expert', None, 'tensor'), may hold values from -0.09375 to 0.09375
- w_down: bfloat16 [64, 768, 4096], P('expert', 'tensor'), may hold values from -0.21875 to 0.21875
Outputs:
- mixed: bfloat16 [256, 4096], P(('groups', 'expert'), 'tensor'), parts along dimension 0
The draws below stay inside these ranges and needn't reach their ends.
There are 2 independent parts, one for each index of `groups`. The reference program is written for one: setup_inputs(seed, part) draws one part's arguments, and reference() takes and returns one part's arrays. A program takes and returns all parts, laid end to end along the dimension named above; an argument that names none is the same for every part. Nothing has to cross between parts.
Inputs may be any that keep to these rules, and one draw needn't show every extreme that they name: `expert_ids`: each row names 8 different experts. Within the 32 rows of one index of the expert axis no expert is named more than 8 times, and in every draw some expert is named exactly 8 times in some such block.
All inputs are finite; a program needn't handle non-finite values.
Results may differ from the reference program's by a relative error of at most 0.014.
Values may be sent and summed in bfloat16 or wider, within the bound.
No kernel may reach another device: no remote copies, remote signals or barrier semaphores. Data moves between devices by JAX's collectives and lax.ppermute only.
A program may use at most 128 MiB of HBM per device.

```python
import math
import jax
import jax.numpy as jnp
import numpy as np
from jax import lax

D = 4096
FF = 768
EXPERTS = 64
TOP = 8
TOK_DEV = 32
CAP = 8
TOKENS = 128
N_TENSOR = 4


def plant(result, rng, smallest, top_value):
    longest = result.shape.index(max(result.shape))
    spots = []
    for shift in (0, 1):
        where = [jax.random.randint(jax.random.fold_in(rng, axis), (), 0, length) for axis, length in enumerate(result.shape)]
        where[longest] = (where[longest] + shift) % result.shape[longest]
        spots.append(tuple(where))
    return result.at[spots[0]].set(smallest).at[spots[1]].set(top_value)


def block_scale(rng, extent, shards, least, top_value):
    factor_of, own = 1.0, jax.random.fold_in(rng, 6)
    for axis_at, parts in shards:
        steps = jnp.exp(jax.random.uniform(jax.random.fold_in(own, axis_at), (parts,), jnp.float32, least / len(shards), top_value / len(shards)))
        factor_of = factor_of * jnp.repeat(steps, extent[axis_at] // parts).reshape([-1 if axis == axis_at else 1 for axis in range(len(extent))])
    return factor_of


def deal_out(rng, own, number, rows, number_of, top, most, lean):
    order = jax.random.permutation(rng, number_of)
    crowded, usual = portions_of(number_of, rows * top, most, lean, True), portions_of(number_of, rows * top, most, lean, False)
    places = jnp.arange(number_of)

    def named(sizes, rotation):
        used = int((sizes > 0).sum())
        fixed = max(1, used // 4)
        shifted = fixed + (places - fixed + rotation * (used - fixed)) % max(1, number_of - fixed)
        return jnp.zeros((number_of,), jnp.int32).at[order[jnp.where(places < fixed, places, shifted)]].set(jnp.asarray(sizes, jnp.int32))

    sizes = jnp.where(number % 4 == 0, named(crowded, number // 4), named(usual, number - number // 4 - 1))
    mixed = jax.random.permutation(jax.random.fold_in(own, 3), number_of)
    source_of, sink = mixed[0:number_of // 2 * 2:2], mixed[1:number_of // 2 * 2:2]
    slack = jnp.minimum(sizes[source_of] - 1, most - sizes[sink]) // 2
    slack = jnp.where((source_of == order[0]) | (sink == order[0]) | (sizes[sink] == 0), 0, jnp.maximum(slack, 0))
    shifted = jax.random.randint(jax.random.fold_in(own, 4), (number_of // 2,), 0, 1 << 20) % (slack + 1)
    sizes = sizes.at[source_of].add(-shifted).at[sink].add(shifted)
    items = jnp.searchsorted(jnp.cumsum(sizes), jnp.arange(rows * top), side="right").astype(jnp.int32)
    table = items.reshape(top, rows).T
    table = table[jax.random.permutation(jax.random.fold_in(own, 1), rows)]
    rotation = jax.random.randint(jax.random.fold_in(own, 2), (rows, 1), 0, top)
    return jnp.take_along_axis(table, (jnp.arange(top)[None, :] + rotation) % top, axis=1)


def portions_of(amount, total, reach, skew, full):
    loads = [(1 << 20) // math.isqrt(rank ** skew) + 1 for rank in range(1, amount + 1)]
    largest = reach if full else min(reach, max(-(-total // amount), total * loads[0] // sum(loads)))
    least = 1 if total - largest >= amount - 1 else 0
    counts, rest = [largest] + [least] * (amount - 1), total - largest - least * (amount - 1)
    while rest > 0:
        free = [i for i in range(1, amount) if counts[i] < largest] or [i for i in range(1, amount) if counts[i] < reach]
        pool, left = sum([loads[i] for i in free]), rest
        for i in free:
            extra = min(reach - counts[i], max(1, left * loads[i] // pool), rest)
            counts[i] = counts[i] + extra
            rest = rest - extra
    return np.array(counts)


def gaussian(stream_key, extent, width, bound, pieces=(), kind=jnp.bfloat16):
    level = block_scale(stream_key, extent, pieces, -0.22, 0.18) if pieces else 1.0
    entries = jax.random.normal(stream_key, extent, jnp.float32) * width * level
    return jnp.minimum(jnp.maximum(entries, -bound), bound).astype(kind)


def setup_inputs(seed: int = 0, part: int = 0) -> dict:
    key_list = jax.random.split(jax.random.key(seed), 7)
    part_splits = jax.random.split(jax.random.fold_in(key_list[6], part), 7)
    tokens = gaussian(part_splits[0], (TOKENS, D), 1.0, 6.0, ((0, 4), (1, 4)))
    expert_ids_keys = jax.random.split(jax.random.fold_in(part_splits[1], 1), TOKENS // TOK_DEV)
    expert_ids_turns = jax.random.permutation(jax.random.fold_in(part_splits[1], 3), TOKENS // TOK_DEV)
    expert_ids = jax.vmap(lambda own, number: deal_out(jax.random.fold_in(part_splits[1], 2), own, number, TOK_DEV, EXPERTS, TOP, CAP, 2))(expert_ids_keys, expert_ids_turns).reshape((TOKENS, TOP))
    gate_fixed = plant(jax.random.randint(part_splits[2], (TOKENS, TOP), 1, 65536), jax.random.fold_in(part_splits[2], 1), 1, 65535).astype(jnp.int32)
    w_gate = gaussian(key_list[3], (EXPERTS, D, FF), D ** -0.5, 0.09375, ((0, 4), (2, 4)))
    w_up = gaussian(key_list[4], (EXPERTS, D, FF), D ** -0.5, 0.09375, ((0, 4), (2, 4)))
    w_down = gaussian(key_list[5], (EXPERTS, FF, D), FF ** -0.5, 0.21875, ((0, 4), (1, 4)))
    return dict(tokens=tokens, expert_ids=expert_ids, gate_fixed=gate_fixed, w_gate=w_gate, w_up=w_up, w_down=w_down)


def reference(tokens, expert_ids, gate_fixed, w_gate, w_up, w_down):
    weights = gate_fixed.astype(jnp.float32)
    gate_share = weights / jnp.sum(weights, axis=1, keepdims=True)
    group_width = FF // N_TENSOR

    def one_expert(running, expert_index):
        chosen = jnp.sum(jnp.where(expert_ids == expert_index, gate_share, jnp.zeros_like(gate_share)), axis=1)
        gate_proj = jnp.dot(tokens, w_gate[expert_index], preferred_element_type=jnp.float32)
        up_proj = jnp.dot(tokens, w_up[expert_index], preferred_element_type=jnp.float32)
        hidden = (jax.nn.silu(gate_proj) * up_proj).astype(jnp.bfloat16)
        down = w_down[expert_index]
        summed = jnp.zeros((tokens.shape[0], D), jnp.float32)
        for piece_index in range(N_TENSOR):
            lower = piece_index * group_width
            group_term = jnp.dot(hidden[:, lower:lower + group_width], down[lower:lower + group_width], preferred_element_type=jnp.float32)
            summed = summed + lax.optimization_barrier(group_term.astype(jnp.bfloat16)).astype(jnp.float32)
        expert_out = lax.optimization_barrier(summed.astype(jnp.bfloat16)).astype(jnp.float32)
        return running + chosen[:, None] * expert_out, None

    start = jnp.zeros((tokens.shape[0], D), jnp.float32)
    running, unused = lax.scan(one_expert, start, jnp.arange(EXPERTS, dtype=jnp.int32))
    return running.astype(jnp.bfloat16)
```

```python
import jax
import jax.numpy as jnp
from jax import lax
from jax.sharding import PartitionSpec as P


def swap(value, axis, step):
    count = lax.axis_size(axis)
    return lax.ppermute(value, axis, [(i, i ^ step) for i in range(count)])


def gather_rows(value, axis):
    return jnp.concatenate([value] + [swap(value, axis, j) for j in range(1, lax.axis_size(axis))], axis=0)


def scatter_rows(value, axis):
    count = lax.axis_size(axis)
    rows = value.shape[0] // count
    total = value[:rows]
    for j in range(1, count):
        block = value[j * rows:(j + 1) * rows].astype(jnp.bfloat16)
        total = total + swap(block, axis, j).astype(jnp.float32)
    return total


def on_device(tokens, expert_ids, gate_fixed, w_gate, w_up, w_down):
    per_token = expert_ids.shape[1]
    local_experts, model, units = w_gate.shape
    width = tokens.shape[1]
    devices_e = lax.axis_size("expert")
    devices_t = lax.axis_size("tensor")
    place_e = lax.axis_index("expert")
    place_t = lax.axis_index("tensor")
    few = devices_e <= 8

    routing = jnp.concatenate([expert_ids, gate_fixed], axis=1)
    if few:
        own = gather_rows(tokens, "expert")
        routing = gather_rows(routing, "expert")
    else:
        own = lax.all_gather(tokens, "expert", axis=0, tiled=True)
        routing = lax.all_gather(routing, "expert", axis=0, tiled=True)
    rows = own.shape[0]

    parts = {0: own}
    bit = devices_t >> 1
    while bit:
        for j in list(parts):
            parts[j ^ bit] = swap(parts[j], "tensor", bit)
        bit >>= 1

    ids = routing[:, :per_token]
    weights = routing[:, per_token:].astype(jnp.float32)
    gate_share = weights / jnp.sum(weights, axis=1, keepdims=True)
    mine = place_e * local_experts + jnp.arange(local_experts, dtype=jnp.int32)
    chosen = jnp.sum(
        jnp.where(ids.T[None, :, :] == mine[:, None, None], gate_share.T[None, :, :], 0.0), axis=1
    )

    gate_rows = jnp.swapaxes(w_gate, 1, 2).reshape(local_experts * units, model)
    up_rows = jnp.swapaxes(w_up, 1, 2).reshape(local_experts * units, model)
    down_rows = w_down.reshape(local_experts * units, model)

    def project(matrix):
        total = None
        for j in sorted(parts):
            piece = lax.dynamic_slice_in_dim(matrix, (place_t ^ j) * width, width, axis=1)
            term = lax.dot_general(
                piece, parts[j], (((1,), (1,)), ((), ())), preferred_element_type=jnp.float32
            )
            total = term if total is None else total + term
        return total

    gate_proj = project(gate_rows)
    up_proj = project(up_rows)
    hidden = (jax.nn.silu(gate_proj) * up_proj).reshape(local_experts, units, rows)
    hidden = (hidden * chosen[:, None, :]).astype(jnp.bfloat16).reshape(local_experts * units, rows)

    def down(j):
        piece = lax.dynamic_slice_in_dim(down_rows, (place_t ^ j) * width, width, axis=1)
        return lax.dot_general(hidden, piece, (((0,), (0,)), ((), ())), preferred_element_type=jnp.float32)

    sums = {j: down(j) for j in sorted(parts, reverse=True)}
    bit = 1
    while bit < devices_t:
        for j in sorted(sums, reverse=True):
            if j & bit:
                sums[j ^ bit] = sums[j ^ bit] + swap(sums.pop(j).astype(jnp.bfloat16), "tensor", bit).astype(jnp.float32)
        bit <<= 1
    if few:
        mixed = scatter_rows(sums[0], "expert")
    else:
        mixed = lax.psum_scatter(sums[0].astype(jnp.bfloat16), "expert", scatter_dimension=0, tiled=True)
    return mixed.astype(jnp.bfloat16)


def solution(mesh):
    placed = (
        P(("groups", "expert"), "tensor"),
        P(("groups", "expert"), None),
        P(("groups", "expert"), None),
        P("expert", None, "tensor"),
        P("expert", None, "tensor"),
        P("expert", "tensor", None),
    )
    return jax.shard_map(
        on_device,
        mesh=mesh,
        in_specs=placed,
        out_specs=P(("groups", "expert"), "tensor"),
        check_vma=False,
    )
```

```python
import jax
import jax.numpy as jnp
from jax import lax
from jax.experimental import pallas as pl
from jax.experimental.pallas import tpu as pltpu
from jax.sharding import PartitionSpec as P


def project_step(x, gate_in, up_in, chosen, w_gate, w_up, first, last, outs, block, units):
    at = pl.multiple_of(pl.program_id(0) * block, block)
    dims = (((1,), (1,)), ((), ()))
    gate = lax.dot_general(w_gate[...], x[...], dims, preferred_element_type=jnp.float32)
    up = lax.dot_general(w_up[...], x[...], dims, preferred_element_type=jnp.float32)
    if not first:
        gate = gate + gate_in[pl.ds(at, block), :]
        up = up + up_in[pl.ds(at, block), :]
    if not last:
        outs[0][pl.ds(at, block), :] = gate
        outs[1][pl.ds(at, block), :] = up
        return
    value = gate / (1.0 + jnp.exp(-gate)) * up
    for k in range(block // units):
        share = chosen[pl.ds(pl.program_id(0) * (block // units) + k, 1), :]
        outs[0][pl.ds(at + k * units, units), :] = (value[k * units:(k + 1) * units] * share).astype(jnp.bfloat16)


def project(index, x, sums, chosen, gate_rows, up_rows, units):
    rows, model = gate_rows.shape
    tokens, width = x.shape
    first, last = sums is None, chosen is not None
    block = units * max(n for n in (1, 2, 3, 4) if (rows // units) % n == 0 and n * units <= 384)
    whole = pl.BlockSpec(memory_space=pltpu.VMEM)
    weight = pl.BlockSpec((block, width), lambda i, place: (i, place[0]))
    extra = ([] if first else list(sums)) + ([chosen] if last else [])

    def body(place, x_ref, *refs):
        refs = list(refs)
        gate_in, up_in = (None, None) if first else (refs.pop(0), refs.pop(0))
        chosen_ref = refs.pop(0) if last else None
        w_gate, w_up = refs.pop(0), refs.pop(0)
        project_step(x_ref, gate_in, up_in, chosen_ref, w_gate, w_up, first, last, refs, block, units)

    wide = jax.ShapeDtypeStruct((rows, tokens), jnp.float32)
    return pl.pallas_call(
        body,
        grid_spec=pltpu.PrefetchScalarGridSpec(
            num_scalar_prefetch=1,
            grid=(rows // block,),
            in_specs=[whole] * (1 + len(extra)) + [weight, weight],
            out_specs=whole if last else [whole, whole],
        ),
        out_shape=jax.ShapeDtypeStruct((rows, tokens), jnp.bfloat16) if last else [wide, wide],
        input_output_aliases={} if first or last else {2: 0, 3: 1},
        compiler_params=pltpu.CompilerParams(dimension_semantics=("arbitrary",), vmem_limit_bytes=24 << 20),
    )(index, x, *extra, gate_rows, up_rows)


def swap(value, axis, step):
    count = lax.axis_size(axis)
    return lax.ppermute(value, axis, [(i, i ^ step) for i in range(count)])


def gather_rows(value, axis):
    return jnp.concatenate([value] + [swap(value, axis, j) for j in range(1, lax.axis_size(axis))], axis=0)


def scatter_rows(value, axis):
    count = lax.axis_size(axis)
    rows = value.shape[0] // count
    total = value[:rows]
    for j in range(1, count):
        block = value[j * rows:(j + 1) * rows].astype(jnp.bfloat16)
        total = total + swap(block, axis, j).astype(jnp.float32)
    return total


def contract(index, hidden, down_rows, width):
    def body(place, hidden_ref, down_ref, out):
        at = pl.multiple_of(place[0] * width, width)
        out[...] = lax.dot_general(
            hidden_ref[...], down_ref[:, pl.ds(at, width)], (((0,), (0,)), ((), ())),
            preferred_element_type=jnp.float32,
        )

    whole = pl.BlockSpec(memory_space=pltpu.VMEM)
    return pl.pallas_call(
        body,
        grid_spec=pltpu.PrefetchScalarGridSpec(
            num_scalar_prefetch=1, grid=(1,), in_specs=[whole, whole], out_specs=whole
        ),
        out_shape=jax.ShapeDtypeStruct((hidden.shape[1], width), jnp.float32),
        compiler_params=pltpu.CompilerParams(vmem_limit_bytes=12 << 20),
    )(index, hidden, down_rows)


def on_device(tokens, expert_ids, gate_fixed, w_gate, w_up, w_down):
    per_token = expert_ids.shape[1]
    local_experts, model, units = w_gate.shape
    width = tokens.shape[1]
    devices_e = lax.axis_size("expert")
    devices_t = lax.axis_size("tensor")
    place_e = lax.axis_index("expert")
    place_t = lax.axis_index("tensor")
    few = devices_e <= 8
    down_rows = w_down.reshape(local_experts * units, model)
    fits = devices_e * tokens.shape[0] <= 256

    routing = jnp.concatenate([expert_ids, gate_fixed], axis=1)
    if few:
        blocks = [tokens] + [swap(tokens, "expert", j) for j in range(1, devices_e)]
        own = jnp.concatenate(blocks, axis=0)
        routing = gather_rows(routing, "expert")
    else:
        own = lax.all_gather(tokens, "expert", axis=0, tiled=True)
        routing = lax.all_gather(routing, "expert", axis=0, tiled=True)
    rows = own.shape[0]

    parts = {0: own}
    for j in range(1, devices_t):
        if j & (j - 1) == 0:
            parts[j] = swap(own, "tensor", j)

    ids = routing[:, :per_token]
    weights = routing[:, per_token:].astype(jnp.float32)
    gate_share = weights / jnp.sum(weights, axis=1, keepdims=True)
    mine = place_e * local_experts + jnp.arange(local_experts, dtype=jnp.int32)
    chosen = jnp.sum(
        jnp.where(ids.T[None, :, :] == mine[:, None, None], gate_share.T[None, :, :], 0.0), axis=1
    )

    gate_rows = jnp.swapaxes(w_gate, 1, 2).reshape(local_experts * units, model)
    up_rows = jnp.swapaxes(w_up, 1, 2).reshape(local_experts * units, model)
    gate_rows = pltpu.with_memory_space_constraint(gate_rows, pltpu.HBM)
    up_rows = pltpu.with_memory_space_constraint(up_rows, pltpu.HBM)

    sums = None
    for j in range(devices_t):
        onward = [c for c in range(j + 1, devices_t) if j and c & (c - 1) == j]
        if onward:
            parts[j], sums = lax.optimization_barrier((parts[j], sums))
            for c in onward:
                parts[c] = swap(parts[j], "tensor", c ^ j)
        index = (place_t ^ j).astype(jnp.int32).reshape(1)
        sums = project(index, parts[j], sums, chosen if j == devices_t - 1 else None, gate_rows, up_rows, units)
    hidden = sums

    def down(j):
        if fits:
            return contract((place_t ^ j).astype(jnp.int32).reshape(1), hidden, down_rows, width)
        piece = lax.dynamic_slice_in_dim(down_rows, (place_t ^ j) * width, width, axis=1)
        return lax.dot_general(hidden, piece, (((0,), (0,)), ((), ())), preferred_element_type=jnp.float32)

    order = sorted(parts, reverse=True)
    sums = {j: down(j) for j in order}
    bit = 1
    while bit < devices_t:
        for j in sorted(sums, reverse=True):
            if j & bit:
                sums[j ^ bit] = sums[j ^ bit] + swap(sums.pop(j).astype(jnp.bfloat16), "tensor", bit).astype(jnp.float32)
        bit <<= 1
    if few:
        mixed = scatter_rows(sums[0], "expert")
    else:
        mixed = lax.psum_scatter(sums[0].astype(jnp.bfloat16), "expert", scatter_dimension=0, tiled=True)
    return mixed.astype(jnp.bfloat16)


def solution(mesh):
    placed = (
        P(("groups", "expert"), "tensor"),
        P(("groups", "expert"), None),
        P(("groups", "expert"), None),
        P("expert", None, "tensor"),
        P("expert", None, "tensor"),
        P("expert", "tensor", None),
    )
    return jax.shard_map(
        on_device,
        mesh=mesh,
        in_specs=placed,
        out_specs=P(("groups", "expert"), "tensor"),
        check_vma=False,
    )
```
